32 devices in a mesh: dp: 8 (over z, y), mp: 4 (over x, core).
Axes of the slice: x: 2, y: 2, z: 4, core: 2. Of those that a mesh axis runs over, the one named last changes fastest.
Arguments:
- hidden: bfloat16 [1024, 7168], P('dp', 'mp'), may hold values from -40 to 40
- live: int32 [1024], P('dp'), may hold values 0 or 1
- norm_gain: float32 [7168], replicated, may hold values from 0.25 to 1.75
- q_weight: bfloat16 [7168, 1536], P(None, 'mp'), may hold values from -0.28347335 to 0.28347335
- kv_weight: bfloat16 [7168, 512], P(None, 'mp'), may hold values from -0.28347335 to 0.28347335
- ratio_ids: int32 [4], replicated, may hold values from 0 to 19
Outputs:
- losses: float32 [4], replicated
- q_latent: bfloat16 [1024, 1536], P('dp', 'mp')
- kv_latent: bfloat16 [1024, 512], P('dp', 'mp')
- feature_means: float32 [7168], replicated
The draws below stay inside these ranges and needn't reach their ends.
All inputs are finite; a program needn't handle non-finite values. No bound on the sum of `live` on one device may be relied on, other than what follows from the above.
Results may differ from the reference program's by a relative error of at most 0.0052.
Values may be sent and summed in bfloat16 or wider, within the bound.
No kernel may reach another device: no remote copies, remote signals or barrier semaphores. Data moves between devices by JAX's collectives and lax.ppermute only.
A program may use at most 256 MiB of HBM per device.

```python
import jax
import jax.numpy as jnp
from jax import lax

D = 7168
QR = 1536
KVR = 512
GROUP = 128
GRID = 20
RATIOS = 4
TOKENS = 1024


def draw_hidden(key, part):
    key_cols = jax.random.fold_in(key, 11)
    key_vals = jax.random.fold_in(key, 12)
    key_boost = jax.random.fold_in(key, 14)
    column_scale = jnp.exp(jax.random.uniform(key_cols, (D,), jnp.float32, -1.2, 1.2))
    boosted = (jax.random.randint(key_boost, (D,), 0, 8) == 0).astype(jnp.float32)
    position = jnp.arange(TOKENS, dtype=jnp.float32) / TOKENS
    strength = 1.0 + 4.0 * (1.0 - position)
    factor = 1.0 + boosted[None, :] * (strength[:, None] - 1.0)
    entries = jax.random.normal(key_vals, (TOKENS, D), jnp.float32) * column_scale[None, :]
    return jnp.clip(entries * factor, -40.0, 40.0).astype(jnp.bfloat16)


def planted_weight(key, columns):
    key_base = jax.random.fold_in(key, 1)
    key_hits = jax.random.fold_in(key, 2)
    key_sign = jax.random.fold_in(key, 3)
    key_size = jax.random.fold_in(key, 4)
    base = jnp.clip(jax.random.normal(key_base, (D, columns), jnp.float32), -6.0, 6.0)
    hits = jax.random.randint(key_hits, (D, columns), 0, 256) == 0
    sign = (2 * jax.random.randint(key_sign, (D, columns), 0, 2) - 1).astype(jnp.float32)
    amplitude = 3.0 + 9.0 * jnp.arange(columns, dtype=jnp.float32) / max(columns - 1, 1)
    size = amplitude[None, :] * (1.0 + jax.random.uniform(key_size, (D, columns), jnp.float32))
    entries = jnp.where(hits, sign * size, base) / jnp.sqrt(jnp.float32(D))
    return entries.astype(jnp.bfloat16)


def draw_q_weight(key, part):
    return planted_weight(jax.random.fold_in(key, 21), QR)


def draw_kv_weight(key, part):
    return planted_weight(jax.random.fold_in(key, 31), KVR)


def place_ends(values, key, low, high):
    longest = values.shape.index(max(values.shape))
    spots = []
    for shift in (0, 1):
        where = [jax.random.randint(jax.random.fold_in(key, axis), (), 0, length) for axis, length in enumerate(values.shape)]
        where[longest] = (where[longest] + shift) % values.shape[longest]
        spots.append(tuple(where))
    return values.at[spots[0]].set(low).at[spots[1]].set(high)


def setup_inputs(seed: int = 0) -> dict:
    key_list = jax.random.split(jax.random.key(seed), 7)
    return {
        "hidden": draw_hidden(jax.random.fold_in(key_list[6], 71), 0),
        "live": place_ends((jax.random.randint(key_list[1], (TOKENS,), 0, 8) < 7).astype(jnp.int32), jax.random.fold_in(key_list[1], 1), 0, 1),
        "norm_gain": jnp.clip(1.0 + 0.15 * jax.random.normal(key_list[2], (D,), jnp.float32), 0.25, 1.75),
        "q_weight": draw_q_weight(jax.random.fold_in(key_list[6], 71), 0),
        "kv_weight": draw_kv_weight(jax.random.fold_in(key_list[6], 71), 0),
        "ratio_ids": place_ends(jax.random.randint(key_list[5], (RATIOS,), 0, GRID), jax.random.fold_in(key_list[5], 1), 0, GRID - 1).astype(jnp.int32),
    }


def fake_quant(weights, scales):
    height, columns = weights.shape
    scaled = weights.astype(jnp.float32) * scales[:, None]
    grouped = scaled.reshape(height // GROUP, GROUP, columns)
    unit_size = (lax.optimization_barrier(jnp.max(jnp.abs(grouped), axis=1, keepdims=True)) + 1e-06) / 7.0
    levels = grouped / unit_size
    stairs = (levels - jnp.sin(2.0 * jnp.pi * levels) / (2.0 * jnp.pi)) * unit_size
    return (stairs.reshape(height, columns) / scales[:, None]).astype(jnp.bfloat16)

def ratio_scales(totals, ratio_ids):
    logged = jnp.log(totals + 1e-06)
    centred = logged - 0.5 * (jnp.max(logged) + jnp.min(logged))
    alphas = ratio_ids.astype(jnp.float32) / GRID
    return jnp.exp(alphas[:, None] * centred[None, :])

def reference(hidden, live, norm_gain, q_weight, kv_weight, ratio_ids):
    values = hidden.astype(jnp.float32)
    mean_square = lax.optimization_barrier(jnp.mean(values * values, axis=1, keepdims=True))
    normed = (values * lax.rsqrt(mean_square + 1e-06) * norm_gain[None, :]).astype(jnp.bfloat16)
    weights = jnp.concatenate([q_weight, kv_weight], axis=1)
    live_rows = live.astype(jnp.float32)[:, None]
    totals = lax.optimization_barrier(jnp.sum(jnp.abs(normed.astype(jnp.float32)) * live_rows, axis=0))
    scales = ratio_scales(totals, ratio_ids)
    exact = jnp.dot(normed, weights, preferred_element_type=jnp.float32)
    energy = jnp.sum((exact * live_rows) ** 2)
    approxes = []
    errors = []
    for position in range(RATIOS):
        quantized = fake_quant(weights, scales[position])
        approx = jnp.dot(normed, quantized, preferred_element_type=jnp.float32)
        errors.append(jnp.sum(((approx - exact) * live_rows) ** 2))
        approxes.append(approx)
    losses = jnp.stack(errors) / energy
    inverse = 1.0 / (losses * losses)
    shares = inverse / jnp.sum(inverse)
    blended = jnp.zeros_like(exact)
    for position in range(RATIOS):
        blended = blended + shares[position] * approxes[position]
    blended = blended.astype(jnp.bfloat16)
    feature_means = totals / TOKENS
    return (losses, blended[:, :QR], blended[:, QR:], feature_means)
```

```python
import functools

import jax
import jax.numpy as jnp
from jax import lax
from jax.experimental import pallas as pl
from jax.experimental.pallas import tpu as pltpu
from jax.sharding import PartitionSpec as P

GROUP = 128
GRID = 20
RATIOS = 4
LANES = 128
BLOCK = 256
SERIES = (6.579656345395702, -12.978563343532759, 12.029937765720488, -5.563853216984216)


def swap(x, axis, distance):
    size = lax.axis_size(axis)
    return lax.ppermute(x, axis, [(i, i ^ distance) for i in range(size)])


def distances(axis):
    size = lax.axis_size(axis)
    assert size & (size - 1) == 0
    return [1 << bit for bit in range(size.bit_length() - 1)]


def total(x, axis):
    for distance in distances(axis):
        x = x + swap(x, axis, distance)
    return x


def slots(x, axis):
    blocks, order = [x], [0]
    for distance in reversed(distances(axis)):
        blocks = blocks + [swap(block, axis, distance) for block in blocks]
        order = order + [distance ^ place for place in order]
    return blocks, order


def column(row):
    return jnp.transpose(jnp.broadcast_to(row, (LANES, LANES)))


def project_kernel(order, tokens, *refs):
    count = len(order)
    me, ids, squares, live, gain = refs[:5]
    hidden = refs[5 : 5 + count]
    totals = refs[5 + count : 5 + 2 * count]
    q_ref, kv_ref = refs[5 + 2 * count : 7 + 2 * count]
    exact, approx, sums, means = refs[7 + 2 * count : 11 + 2 * count]
    normed, scales, table, stretched, shrunk, quant = refs[11 + 2 * count :]
    step = pl.program_id(0)
    rows = hidden[0].shape[0]
    width = hidden[0].shape[1]
    features = width * count
    per_slot = width // LANES

    @pl.when(step == 0)
    def _():
        for slot in range(count):
            owner = me[0] ^ order[slot]
            for piece in range(per_slot):
                means[pl.ds(owner * per_slot + piece, 1), :] = totals[slot][piece : piece + 1, :]
        sums_all = means[...]
        logged = jnp.log(sums_all + 1e-06)
        centred = logged - 0.5 * (jnp.max(logged) + jnp.min(logged))
        means[...] = sums_all / tokens
        for ratio in range(RATIOS):
            alpha = ids[ratio].astype(jnp.float32) / GRID
            scale = jnp.exp(alpha * centred)
            scales[:, ratio, :] = scale
            scales[:, RATIOS + ratio, :] = 1.0 / scale
        for top in range(0, rows, LANES):
            mean_square = squares[:, top : top + LANES] / features
            rooted = column(lax.rsqrt(mean_square + 1e-06))
            for slot in range(count):
                owner = me[0] ^ order[slot]
                for piece in range(per_slot):
                    place = owner * per_slot + piece
                    values = hidden[slot][top : top + LANES, piece * LANES : (piece + 1) * LANES]
                    values = values.astype(jnp.float32) * rooted * gain[pl.ds(place, 1), :]
                    normed[place, top : top + LANES, :] = values.astype(jnp.bfloat16)
        exact[...] = jnp.zeros_like(exact)
        approx[...] = jnp.zeros_like(approx)

    groups = BLOCK // GROUP
    parts = [(q_ref, at) for at in range(0, q_ref.shape[1], LANES)]
    parts += [(kv_ref, at) for at in range(0, kv_ref.shape[1], LANES)]
    for group in range(groups):
        table[...] = jnp.transpose(scales[step * groups + group])
        for ratio in range(RATIOS):
            stretched[ratio] = jnp.broadcast_to(table[:, ratio : ratio + 1], (LANES, LANES))
            shrunk[ratio] = jnp.broadcast_to(
                table[:, RATIOS + ratio : RATIOS + ratio + 1], (LANES, LANES)
            ).astype(jnp.bfloat16)
        for spot, (ref, at) in enumerate(parts):
            weight = ref[group * GROUP : (group + 1) * GROUP, at : at + LANES]
            wide = weight.astype(jnp.float32)
            for ratio in range(RATIOS):
                scaled = wide * stretched[ratio]
                peak = jnp.max(jnp.abs(scaled), axis=0, keepdims=True)
                unit = (peak + 1e-06) / 7.0
                level = scaled * (1.0 / unit)
                part = (level - jnp.round(level)).astype(jnp.bfloat16)
                square = part * part
                series = jnp.full_like(square, SERIES[-1])
                for term in SERIES[-2::-1]:
                    series = series * square + jnp.bfloat16(term)
                wave = part - part * square * series
                wave = wave * unit.astype(jnp.bfloat16) * shrunk[ratio]
                quant[ratio, group * GROUP : (group + 1) * GROUP, spot * LANES : (spot + 1) * LANES] = weight - wave
    left = jnp.concatenate([normed[step * groups + group] for group in range(groups)], axis=1)
    for ratio in range(RATIOS):
        approx[ratio] += jnp.dot(left, quant[ratio], preferred_element_type=jnp.float32)
    query = q_ref.shape[1]
    exact[:, :query] += jnp.dot(left, q_ref[...], preferred_element_type=jnp.float32)
    exact[:, query:] += jnp.dot(left, kv_ref[...], preferred_element_type=jnp.float32)

    @pl.when(step == pl.num_programs(0) - 1)
    def _():
        masks = [column(live[:, top : top + LANES].astype(jnp.float32)) for top in range(0, rows, LANES)]
        for ratio in range(RATIOS + 1):
            gathered = jnp.zeros((1, LANES), jnp.float32)
            for index, top in enumerate(range(0, rows, LANES)):
                for at in range(0, exact.shape[1], LANES):
                    value = exact[top : top + LANES, at : at + LANES]
                    if ratio < RATIOS:
                        value = approx[ratio, top : top + LANES, at : at + LANES] - value
                    value = value * masks[index]
                    gathered = gathered + jnp.sum(value * value, axis=0, keepdims=True)
            sums[ratio : ratio + 1, :] = gathered
        sums[RATIOS + 1 :, :] = jnp.zeros((8 - RATIOS - 1, LANES), jnp.float32)


def blend_kernel(sums, approx, losses, query, kv):
    folded = [jnp.sum(sums[ratio : ratio + 1, :], axis=1, keepdims=True) for ratio in range(RATIOS + 1)]
    loss = [folded[ratio] / folded[RATIOS] for ratio in range(RATIOS)]
    inverse = [1.0 / (value * value) for value in loss]
    whole = inverse[0] + inverse[1] + inverse[2] + inverse[3]
    for ratio in range(RATIOS):
        losses[ratio : ratio + 1, :] = jnp.broadcast_to(loss[ratio], (1, LANES))
    blended = (inverse[0] / whole) * approx[0]
    for ratio in range(1, RATIOS):
        blended = blended + (inverse[ratio] / whole) * approx[ratio]
    blended = blended.astype(jnp.bfloat16)
    query[...] = blended[:, : query.shape[1]]
    kv[...] = blended[:, query.shape[1] :]


def per_device(hidden, live, norm_gain, q_weight, kv_weight, ratio_ids):
    rows, width = hidden.shape
    shards = lax.axis_size("mp")
    features = width * shards
    tokens = rows * lax.axis_size("dp")
    query, kv = q_weight.shape[1], kv_weight.shape[1]
    me = lax.axis_index("mp")

    values = hidden.astype(jnp.float32)
    squares = total(jnp.sum(values * values, axis=1).reshape(1, rows), "mp")
    gain_slice = lax.dynamic_slice_in_dim(norm_gain, me * width, width)
    scaling = lax.rsqrt(squares.reshape(rows, 1) / features + 1e-06)
    own = (values * scaling * gain_slice[None, :]).astype(jnp.bfloat16)
    live_rows = live.astype(jnp.float32)[:, None]
    sums = jnp.sum(jnp.abs(own.astype(jnp.float32)) * live_rows, axis=0)
    sums = total(sums.reshape(width // LANES, LANES), "dp")
    total_slots, order = slots(sums, "mp")
    hidden_slots, _ = slots(hidden, "mp")

    whole = lambda shape: pl.BlockSpec(shape, lambda i: (0,) * len(shape))
    scalar = pl.BlockSpec(memory_space=pltpu.SMEM)
    exact, approx, sums, means = pl.pallas_call(
        functools.partial(project_kernel, tuple(order), float(tokens)),
        grid=(features // BLOCK,),
        in_specs=[scalar, scalar, whole((1, rows)), whole((1, rows)), whole((features // LANES, LANES))]
        + [whole((rows, width))] * shards
        + [whole((width // LANES, LANES))] * shards
        + [
            pl.BlockSpec((BLOCK, query), lambda i: (i, 0)),
            pl.BlockSpec((BLOCK, kv), lambda i: (i, 0)),
        ],
        out_specs=[
            whole((rows, query + kv)),
            whole((RATIOS, rows, query + kv)),
            whole((8, LANES)),
            whole((features // LANES, LANES)),
        ],
        out_shape=[
            jax.ShapeDtypeStruct((rows, query + kv), jnp.float32),
            jax.ShapeDtypeStruct((RATIOS, rows, query + kv), jnp.float32),
            jax.ShapeDtypeStruct((8, LANES), jnp.float32),
            jax.ShapeDtypeStruct((features // LANES, LANES), jnp.float32),
        ],
        scratch_shapes=[
            pltpu.VMEM((features // LANES, rows, LANES), jnp.bfloat16),
            pltpu.VMEM((features // LANES, 8, LANES), jnp.float32),
            pltpu.VMEM((LANES, 8), jnp.float32),
            pltpu.VMEM((RATIOS, LANES, LANES), jnp.float32),
            pltpu.VMEM((RATIOS, LANES, LANES), jnp.bfloat16),
            pltpu.VMEM((RATIOS, BLOCK, query + kv), jnp.bfloat16),
        ],
        name="project",
    )(
        me.reshape(1).astype(jnp.int32),
        ratio_ids,
        squares,
        live.reshape(1, rows),
        norm_gain.reshape(features // LANES, LANES),
        *hidden_slots,
        *total_slots,
        q_weight,
        kv_weight,
    )
    sums = total(total(sums, "mp"), "dp")
    losses, q_latent, kv_latent = pl.pallas_call(
        blend_kernel,
        out_shape=[
            jax.ShapeDtypeStruct((RATIOS, LANES), jnp.float32),
            jax.ShapeDtypeStruct((rows, query), jnp.bfloat16),
            jax.ShapeDtypeStruct((rows, kv), jnp.bfloat16),
        ],
        name="blend",
    )(sums, approx)
    return losses[:, 0], q_latent, kv_latent, means.reshape(features)


def solution(mesh):
    placed = (P("dp", "mp"), P("dp"), P(), P(None, "mp"), P(None, "mp"), P())
    return jax.shard_map(
        per_device,
        mesh=mesh,
        in_specs=placed,
        out_specs=(P(), P("dp", "mp"), P("dp", "mp"), P()),
        check_vma=False,
    )
```

```python
import functools

import jax
import jax.numpy as jnp
from jax import lax
from jax.experimental import pallas as pl
from jax.experimental.pallas import tpu as pltpu
from jax.sharding import PartitionSpec as P

GROUP = 128
GRID = 20
RATIOS = 4
LANES = 128
HALF = 256
LINEAR, CONSTANT, GAIN = -1.1640625, 0.458984375, 8.705


def swap(x, axis, distance):
    size = lax.axis_size(axis)
    return lax.ppermute(x, axis, [(i, i ^ distance) for i in range(size)])


def distances(axis):
    size = lax.axis_size(axis)
    assert size & (size - 1) == 0
    return [1 << bit for bit in range(size.bit_length() - 1)]


def total(x, axis):
    for distance in distances(axis):
        x = x + swap(x, axis, distance)
    return x


def peers(x, axis):
    return [x] + [swap(x, axis, distance) for distance in range(1, lax.axis_size(axis))]


def slots(x, axis):
    blocks = {0: x}
    for distance in reversed(distances(axis)):
        blocks.update({place ^ distance: swap(block, axis, distance) for place, block in list(blocks.items())})
    return [blocks[place] for place in range(len(blocks))]


def column(row):
    return jnp.transpose(jnp.broadcast_to(row, (LANES, LANES)))


def norm_kernel(features, *refs):
    me, squares, gain, *hidden, normed = refs
    rows, width = hidden[0].shape
    per_slot = width // LANES
    for top in range(0, rows, LANES):
        mean_square = squares[:, top : top + LANES] / features
        rooted = column(lax.rsqrt(mean_square + 1e-06))
        for slot in range(len(hidden)):
            owner = me[0] ^ slot
            for piece in range(per_slot):
                place = owner * per_slot + piece
                values = hidden[slot][top : top + LANES, piece * LANES : (piece + 1) * LANES]
                values = values.astype(jnp.float32) * rooted * gain[pl.ds(place, 1), :]
                normed[place, top : top + LANES, :] = values.astype(jnp.bfloat16)


def project_kernel(count, tokens, spots, *refs):
    me, ids, live = refs[:3]
    totals = refs[3 : 3 + count]
    normed = refs[3 + count]
    weights = refs[4 + count : 4 + count + spots]
    exact, delta, sums, means = refs[4 + count + spots : 8 + count + spots]
    scales, table, stretched, waves = refs[8 + count + spots :]
    step = pl.program_id(0)
    last = pl.num_programs(0) - 1
    rows = normed.shape[1]
    blocks = normed.shape[0]
    per_slot = blocks // count
    groups = HALF // GROUP

    def prepare(group, buffer):
        table[buffer] = jnp.transpose(scales[group])
        for ratio in range(RATIOS):
            stretched[buffer, ratio] = jnp.broadcast_to(table[buffer, :, ratio : ratio + 1], (LANES, LANES))

    def quantize(half, group, buffer):
        top = half * HALF + group * GROUP
        for spot in range(spots):
            wide = weights[spot][top : top + GROUP, :].astype(jnp.float32)
            for ratio in range(RATIOS):
                scaled = wide * stretched[buffer, ratio]
                peak = jnp.max(jnp.abs(scaled), axis=0, keepdims=True)
                unit = (peak + 1e-06) / 7.0
                level = scaled * (1.0 / unit)
                part = (level - jnp.round(level)).astype(jnp.bfloat16)
                square = part * part
                series = (square + jnp.bfloat16(LINEAR)) * square + jnp.bfloat16(CONSTANT)
                wave = series * (jnp.bfloat16(0.25) - square) * part
                wave = wave * (unit * GAIN).astype(jnp.bfloat16)
                waves[half, ratio, spot, group * GROUP : (group + 1) * GROUP, :] = wave

    def multiply(half, first):
        for ratio in range(RATIOS):
            left = []
            for group in range(groups):
                shrink = scales[first + group, RATIOS + ratio : RATIOS + ratio + 1, :]
                left.append(normed[first + group] * shrink.astype(jnp.bfloat16))
            right = jnp.concatenate([waves[half, ratio, spot] for spot in range(spots)], axis=1)
            delta[ratio] += jnp.dot(jnp.concatenate(left, axis=1), right, preferred_element_type=jnp.float32)

    @pl.when(step == 0)
    def _():
        for slot in range(count):
            owner = me[0] ^ slot
            for piece in range(per_slot):
                means[pl.ds(owner * per_slot + piece, 1), :] = totals[slot][piece : piece + 1, :]
        sums_all = means[...]
        logged = jnp.log(sums_all + 1e-06)
        centred = logged - 0.5 * (jnp.max(logged) + jnp.min(logged))
        means[...] = sums_all / tokens
        for ratio in range(RATIOS):
            alpha = ids[ratio].astype(jnp.float32) / GRID
            scale = jnp.exp(alpha * centred)
            scales[:, ratio, :] = scale
            scales[:, RATIOS + ratio, :] = 1.0 / scale
        exact[...] = jnp.zeros_like(exact)
        delta[...] = jnp.zeros_like(delta)
        waves[1] = jnp.zeros_like(waves[1])
        prepare(0, 0)

    base = step * 2 * groups
    for half in range(2):
        for group in range(groups):
            index = half * groups + group
            prepare(jnp.minimum(base + index + 1, blocks - 1), (index + 1) % 2)
            quantize(half, group, index % 2)
        multiply(1 - half, base if half else jnp.maximum(base - groups, 0))
    for half in range(2):
        left = jnp.concatenate([normed[base + half * groups + group] for group in range(groups)], axis=1)
        right = jnp.concatenate([weight[half * HALF : (half + 1) * HALF, :] for weight in weights], axis=1)
        exact[...] += jnp.dot(left, right, preferred_element_type=jnp.float32)

    @pl.when(step == last)
    def _():
        multiply(1, base + groups)
        masks = [column(live[:, top : top + LANES].astype(jnp.float32)) for top in range(0, rows, LANES)]
        for ratio in range(RATIOS + 1):
            gathered = jnp.zeros((1, LANES), jnp.float32)
            for index, top in enumerate(range(0, rows, LANES)):
                for at in range(0, exact.shape[1], LANES):
                    if ratio < RATIOS:
                        value = delta[ratio, top : top + LANES, at : at + LANES]
                    else:
                        value = exact[top : top + LANES, at : at + LANES]
                    value = value * masks[index]
                    gathered = gathered + jnp.sum(value * value, axis=0, keepdims=True)
            sums[ratio : ratio + 1, :] = gathered
        sums[RATIOS + 1 :, :] = jnp.zeros((8 - RATIOS - 1, LANES), jnp.float32)


def blend_kernel(first, second, exact, delta, losses, query, kv):
    sums = first[...] + second[...]
    folded = [jnp.sum(sums[ratio : ratio + 1, :], axis=1, keepdims=True) for ratio in range(RATIOS + 1)]
    loss = [folded[ratio] / folded[RATIOS] for ratio in range(RATIOS)]
    inverse = [1.0 / (value * value) for value in loss]
    whole = inverse[0]
    for ratio in range(1, RATIOS):
        whole = whole + inverse[ratio]
    blended = exact[...]
    for ratio in range(RATIOS):
        losses[ratio] = loss[ratio][0, 0]
        blended = blended - (inverse[ratio] / whole) * delta[ratio]
    blended = blended.astype(jnp.bfloat16)
    query[...] = blended[:, : query.shape[1]]
    kv[...] = blended[:, query.shape[1] :]


def project(me, ratio_ids, live, total_slots, normed, q_weight, kv_weight, tokens):
    blocks, rows, _ = normed.shape
    features = blocks * LANES
    columns = q_weight.shape[1] + kv_weight.shape[1]
    spots = columns // LANES
    block = 2 * HALF
    whole = lambda shape: pl.BlockSpec(shape, lambda i: (0,) * len(shape))
    scalar = pl.BlockSpec(memory_space=pltpu.SMEM)
    lane_tile = lambda tile: pl.BlockSpec((block, LANES), lambda i: (i, tile))
    weights, tiles = [], []
    for array in (q_weight, kv_weight):
        for tile in range(array.shape[1] // LANES):
            weights.append(array)
            tiles.append(lane_tile(tile))
    return pl.pallas_call(
        functools.partial(project_kernel, len(total_slots), tokens, spots),
        grid=(features // block,),
        in_specs=[scalar, scalar, whole((1, rows))]
        + [whole(part.shape) for part in total_slots]
        + [whole(normed.shape)]
        + tiles,
        out_specs=[
            whole((rows, columns)),
            whole((RATIOS, rows, columns)),
            whole((8, LANES)),
            whole((blocks, LANES)),
        ],
        out_shape=[
            jax.ShapeDtypeStruct((rows, columns), jnp.float32),
            jax.ShapeDtypeStruct((RATIOS, rows, columns), jnp.float32),
            jax.ShapeDtypeStruct((8, LANES), jnp.float32),
            jax.ShapeDtypeStruct((blocks, LANES), jnp.float32),
        ],
        scratch_shapes=[
            pltpu.VMEM((blocks, 8, LANES), jnp.float32),
            pltpu.VMEM((2, LANES, 8), jnp.float32),
            pltpu.VMEM((2, RATIOS, LANES, LANES), jnp.float32),
            pltpu.VMEM((2, RATIOS, spots, HALF, LANES), jnp.bfloat16),
        ],
        cost_estimate=pl.CostEstimate(flops=10 * rows * features * columns, bytes_accessed=8 * features * columns, transcendentals=0),
        name="project",
    )(me, ratio_ids, live, *total_slots, normed, *weights)


def per_device(hidden, live, norm_gain, q_weight, kv_weight, ratio_ids):
    rows, width = hidden.shape
    shards = lax.axis_size("mp")
    features = width * shards
    tokens = rows * lax.axis_size("dp")
    query, kv = q_weight.shape[1], kv_weight.shape[1]
    index = lax.axis_index("mp")
    me = index.reshape(1).astype(jnp.int32)

    values = hidden.astype(jnp.float32)
    squares = sum(peers(jnp.sum(values * values, axis=1).reshape(1, rows), "mp"))
    squares, late = lax.optimization_barrier((squares, hidden))
    hidden_slots = slots(late, "mp")
    gain_slice = lax.dynamic_slice_in_dim(norm_gain, index * width, width)
    scaling = lax.rsqrt(squares.reshape(rows, 1) / features + 1e-06)
    own = (values * scaling * gain_slice[None, :]).astype(jnp.bfloat16)
    live_rows = live.astype(jnp.float32)[:, None]
    sums = jnp.sum(jnp.abs(own.astype(jnp.float32)) * live_rows, axis=0)
    sums = total(sums.reshape(width // LANES, LANES), "dp")
    total_slots = peers(sums, "mp")

    scalar = pl.BlockSpec(memory_space=pltpu.SMEM)
    vector = pl.BlockSpec(memory_space=pltpu.VMEM)
    normed = pl.pallas_call(
        functools.partial(norm_kernel, features),
        in_specs=[scalar] + [vector] * (2 + shards),
        out_specs=vector,
        out_shape=jax.ShapeDtypeStruct((features // LANES, rows, LANES), jnp.bfloat16),
        cost_estimate=pl.CostEstimate(flops=4 * rows * features, bytes_accessed=4 * rows * features, transcendentals=0),
        name="norm",
    )(me, squares, norm_gain.reshape(features // LANES, LANES), *hidden_slots)
    exact, delta, sums, means = project(
        me, ratio_ids, live.reshape(1, rows), total_slots, normed, q_weight, kv_weight, float(tokens)
    )
    sums = sum(peers(sums, "mp"))
    *steps, final = distances("dp")
    for distance in steps:
        sums = sums + swap(sums, "dp", distance)
    losses, q_latent, kv_latent = pl.pallas_call(
        blend_kernel,
        out_shape=[
            jax.ShapeDtypeStruct((RATIOS,), jnp.float32),
            jax.ShapeDtypeStruct((rows, query), jnp.bfloat16),
            jax.ShapeDtypeStruct((rows, kv), jnp.bfloat16),
        ],
        out_specs=[scalar, vector, vector],
        name="blend",
    )(sums, swap(sums, "dp", final), exact, delta)
    return losses, q_latent, kv_latent, means.reshape(features)


def solution(mesh):
    placed = (P("dp", "mp"), P("dp"), P(), P(None, "mp"), P(None, "mp"), P())
    return jax.shard_map(
        per_device,
        mesh=mesh,
        in_specs=placed,
        out_specs=(P(), P("dp", "mp"), P("dp", "mp"), P()),
        check_vma=False,
    )
```

```python
import functools

import jax
import jax.numpy as jnp
from jax import lax
from jax.experimental import pallas as pl
from jax.experimental.pallas import tpu as pltpu
from jax.sharding import PartitionSpec as P

GROUP = 128
GRID = 20
RATIOS = 4
LANES = 128
HALF = 256
LINEAR, CONSTANT, GAIN = -1.1640625, 0.458984375, 8.705


def swap(x, axis, distance):
    size = lax.axis_size(axis)
    return lax.ppermute(x, axis, [(i, i ^ distance) for i in range(size)])


def distances(axis):
    size = lax.axis_size(axis)
    assert size & (size - 1) == 0
    return [1 << bit for bit in range(size.bit_length() - 1)]


def total(x, axis):
    for distance in distances(axis):
        x = x + swap(x, axis, distance)
    return x


def peers(x, axis):
    return [x] + [swap(x, axis, distance) for distance in range(1, lax.axis_size(axis))]


def column(row):
    return jnp.transpose(jnp.broadcast_to(row, (LANES, LANES)))


def squares_kernel(hidden, live, gain, squares, kept, mask, kept_gain):
    kept[...] = hidden[...]
    kept_gain[...] = gain[...]
    mask[...] = live[...].astype(jnp.float32)
    for top in range(0, hidden.shape[0], LANES):
        gathered = jnp.zeros((LANES, LANES), jnp.float32)
        for at in range(0, hidden.shape[1], LANES):
            values = hidden[top : top + LANES, at : at + LANES].astype(jnp.float32)
            gathered = gathered + values * values
        squares[:, top : top + LANES] = jnp.sum(jnp.transpose(gathered), axis=0, keepdims=True)


def stats_kernel(features, me, squares, live, gain, hidden, sums):
    rows, width = hidden.shape
    per_slot = width // LANES
    for piece in range(per_slot):
        row = gain[pl.ds(me[0] * per_slot + piece, 1), :]
        gathered = jnp.zeros((1, LANES), jnp.float32)
        for top in range(0, rows, LANES):
            rooted = column(lax.rsqrt(squares[:, top : top + LANES] / features + 1e-06))
            mask = column(live[:, top : top + LANES])
            values = hidden[top : top + LANES, piece * LANES : (piece + 1) * LANES].astype(jnp.float32)
            values = (values * rooted * row).astype(jnp.bfloat16).astype(jnp.float32)
            gathered = gathered + jnp.sum(jnp.abs(values) * mask, axis=0, keepdims=True)
        sums[piece : piece + 1, :] = gathered


def norm_kernel(features, *refs):
    me, squares, gain, *hidden, normed = refs
    rows, width = hidden[0].shape
    per_slot = width // LANES
    for top in range(0, rows, LANES):
        mean_square = squares[:, top : top + LANES] / features
        rooted = column(lax.rsqrt(mean_square + 1e-06))
        for slot in range(len(hidden)):
            owner = me[0] ^ slot
            for piece in range(per_slot):
                place = owner * per_slot + piece
                values = hidden[slot][top : top + LANES, piece * LANES : (piece + 1) * LANES]
                values = values.astype(jnp.float32) * rooted * gain[pl.ds(place, 1), :]
                normed[place, top : top + LANES, :] = values.astype(jnp.bfloat16)


def project_kernel(count, tokens, *refs):
    me, ids, live = refs[:3]
    totals = refs[3 : 3 + count]
    normed, query, kv = refs[3 + count : 6 + count]
    exact, delta, sums, means = refs[6 + count : 10 + count]
    scales, table, stretched, waves, held, arrivals = refs[10 + count :]
    rows = normed.shape[1]
    blocks = normed.shape[0]
    per_slot = blocks // count
    groups = HALF // GROUP
    parts = [(ref, at) for ref in (query, kv) for at in range(0, ref.shape[1], LANES)]
    steps = blocks // (2 * groups)

    def fetches(step):
        slot = lax.rem(step, 2)
        span = pl.ds(pl.multiple_of(step * 2 * HALF, 2 * HALF), 2 * HALF)
        return [
            pltpu.make_async_copy(ref.at[span, pl.ds(at, LANES)], held.at[slot, spot], arrivals.at[slot, spot])
            for spot, (ref, at) in enumerate(parts)
        ]

    def prepare(group, buffer):
        table[buffer] = jnp.transpose(scales[group])
        for ratio in range(RATIOS):
            stretched[buffer, ratio] = jnp.broadcast_to(table[buffer, :, ratio : ratio + 1], (LANES, LANES))

    def quantize(half, group, buffer, slot):
        top = half * HALF + group * GROUP
        for spot in range(len(parts)):
            wide = held[slot, spot, top : top + GROUP, :].astype(jnp.float32)
            for ratio in range(RATIOS):
                scaled = wide * stretched[buffer, ratio]
                peak = jnp.max(jnp.abs(scaled), axis=0, keepdims=True) + 1e-06
                level = scaled * (7.0 / peak)
                part = (level - jnp.round(level)).astype(jnp.bfloat16)
                square = part * part
                series = (square + jnp.bfloat16(LINEAR)) * square + jnp.bfloat16(CONSTANT)
                wave = series * (jnp.bfloat16(0.25) - square) * part
                wave = wave * (peak * (GAIN / 7.0)).astype(jnp.bfloat16)
                waves[half, ratio, spot, group * GROUP : (group + 1) * GROUP, :] = wave

    def multiply(half, first):
        for ratio in range(RATIOS):
            left = []
            for group in range(groups):
                shrink = scales[first + group, RATIOS + ratio : RATIOS + ratio + 1, :]
                left.append(normed[first + group] * shrink.astype(jnp.bfloat16))
            right = jnp.concatenate([waves[half, ratio, spot] for spot in range(len(parts))], axis=1)
            delta[ratio] += jnp.dot(jnp.concatenate(left, axis=1), right, preferred_element_type=jnp.float32)

    def project_exact(half, first, slot):
        left = jnp.concatenate([normed[first + group] for group in range(groups)], axis=1)
        right = [held[slot, spot, half * HALF : (half + 1) * HALF, :] for spot in range(len(parts))]
        exact[...] += jnp.dot(left, jnp.concatenate(right, axis=1), preferred_element_type=jnp.float32)

    for fetch in fetches(0):
        fetch.start()
    for slot in range(count):
        owner = me[0] ^ slot
        for piece in range(per_slot):
            means[pl.ds(owner * per_slot + piece, 1), :] = totals[slot][piece : piece + 1, :]
    sums_all = means[...]
    logged = jnp.log(sums_all + 1e-06)
    centred = logged - 0.5 * (jnp.max(logged) + jnp.min(logged))
    means[...] = sums_all / tokens
    for ratio in range(RATIOS):
        alpha = ids[ratio].astype(jnp.float32) / GRID
        scale = jnp.exp(alpha * centred)
        scales[:, ratio, :] = scale
        scales[:, RATIOS + ratio, :] = 1.0 / scale
    exact[...] = jnp.zeros_like(exact)
    delta[...] = jnp.zeros_like(delta)
    waves[1] = jnp.zeros_like(waves[1])
    prepare(0, 0)

    @pl.loop(0, steps)
    def _(step):
        base = step * 2 * groups
        slot = lax.rem(step, 2)

        @pl.when(step + 1 < steps)
        def _():
            for fetch in fetches(step + 1):
                fetch.start()

        for fetch in fetches(step):
            fetch.wait()
        for half in range(2):
            first = base + half * groups
            for group in range(groups):
                index = half * groups + group
                prepare(jnp.minimum(base + index + 1, blocks - 1), (index + 1) % 2)
                quantize(half, group, index % 2, slot)
            multiply(1 - half, jnp.maximum(first - groups, 0))
            project_exact(half, first, slot)

    multiply(1, blocks - groups)
    masks = [column(live[:, top : top + LANES]) for top in range(0, rows, LANES)]
    for ratio in range(RATIOS + 1):
        gathered = jnp.zeros((1, LANES), jnp.float32)
        for index, top in enumerate(range(0, rows, LANES)):
            for at in range(0, exact.shape[1], LANES):
                if ratio < RATIOS:
                    value = delta[ratio, top : top + LANES, at : at + LANES]
                else:
                    value = exact[top : top + LANES, at : at + LANES]
                value = value * masks[index]
                gathered = gathered + jnp.sum(value * value, axis=0, keepdims=True)
        sums[ratio : ratio + 1, :] = gathered
    sums[RATIOS + 1 :, :] = jnp.zeros((8 - RATIOS - 1, LANES), jnp.float32)


def blend_kernel(first, second, exact, delta, losses, query, kv):
    sums = first[...] + second[...]
    folded = [jnp.sum(sums[ratio : ratio + 1, :], axis=1, keepdims=True) for ratio in range(RATIOS + 1)]
    loss = [folded[ratio] / folded[RATIOS] for ratio in range(RATIOS)]
    inverse = [1.0 / (value * value) for value in loss]
    whole = inverse[0]
    for ratio in range(1, RATIOS):
        whole = whole + inverse[ratio]
    blended = exact[...]
    for ratio in range(RATIOS):
        losses[ratio] = loss[ratio][0, 0]
        blended = blended - (inverse[ratio] / whole) * delta[ratio]
    blended = blended.astype(jnp.bfloat16)
    query[...] = blended[:, : query.shape[1]]
    kv[...] = blended[:, query.shape[1] :]


SCALAR = pl.BlockSpec(memory_space=pltpu.SMEM)
VECTOR = pl.BlockSpec(memory_space=pltpu.VMEM)


def room(mebibytes):
    return pltpu.CompilerParams(vmem_limit_bytes=mebibytes << 20)


def cost(flops, moved):
    return pl.CostEstimate(flops=flops, bytes_accessed=moved, transcendentals=0)


def project(me, ratio_ids, live, total_slots, normed, q_weight, kv_weight, tokens):
    blocks, rows, _ = normed.shape
    features = blocks * LANES
    columns = q_weight.shape[1] + kv_weight.shape[1]
    spots = columns // LANES
    count = len(total_slots)
    return pl.pallas_call(
        functools.partial(project_kernel, count, tokens),
        in_specs=[SCALAR, SCALAR] + [VECTOR] * (2 + count) + [pl.BlockSpec(memory_space=pl.ANY)] * 2,
        out_specs=[VECTOR] * 4,
        out_shape=[
            jax.ShapeDtypeStruct((rows, columns), jnp.float32),
            jax.ShapeDtypeStruct((RATIOS, rows, columns), jnp.float32),
            jax.ShapeDtypeStruct((8, LANES), jnp.float32),
            jax.ShapeDtypeStruct((blocks, LANES), jnp.float32),
        ],
        scratch_shapes=[
            pltpu.VMEM((blocks, 8, LANES), jnp.float32),
            pltpu.VMEM((2, LANES, 8), jnp.float32),
            pltpu.VMEM((2, RATIOS, LANES, LANES), jnp.float32),
            pltpu.VMEM((2, RATIOS, spots, HALF, LANES), jnp.bfloat16),
            pltpu.VMEM((2, spots, 2 * HALF, LANES), jnp.bfloat16),
            pltpu.SemaphoreType.DMA((2, spots)),
        ],
        compiler_params=room(50),
        cost_estimate=cost(10 * rows * features * columns, 8 * features * columns),
        name="project",
    )(me, ratio_ids, live, *total_slots, normed, q_weight, kv_weight)


def per_device(hidden, live, norm_gain, q_weight, kv_weight, ratio_ids):
    rows, width = hidden.shape
    shards = lax.axis_size("mp")
    features = width * shards
    tokens = rows * lax.axis_size("dp")
    query, kv = q_weight.shape[1], kv_weight.shape[1]
    me = lax.axis_index("mp").reshape(1).astype(jnp.int32)

    squares, hidden, live_row, gain = pl.pallas_call(
        squares_kernel,
        in_specs=[VECTOR] * 3,
        out_specs=[VECTOR] * 4,
        out_shape=[
            jax.ShapeDtypeStruct((1, rows), jnp.float32),
            jax.ShapeDtypeStruct(hidden.shape, hidden.dtype),
            jax.ShapeDtypeStruct((1, rows), jnp.float32),
            jax.ShapeDtypeStruct((features // LANES, LANES), jnp.float32),
        ],
        compiler_params=room(2),
        cost_estimate=cost(2 * rows * width, 4 * rows * width),
        name="squares",
    )(hidden, live.reshape(1, rows), norm_gain.reshape(features // LANES, LANES))
    squares = sum(peers(squares, "mp"))
    squares, late = lax.optimization_barrier((squares, hidden))
    *nearer, farthest = distances("mp")
    held = {0: late, farthest: swap(late, "mp", farthest)}
    for distance in nearer:
        held[distance] = swap(late, "mp", distance)
    sums = pl.pallas_call(
        functools.partial(stats_kernel, features),
        in_specs=[SCALAR] + [VECTOR] * 4,
        out_specs=VECTOR,
        out_shape=jax.ShapeDtypeStruct((width // LANES, LANES), jnp.float32),
        compiler_params=room(2),
        cost_estimate=cost(8 * rows * width, 2 * rows * width),
        name="stats",
    )(me, squares, live_row, gain, hidden)
    sums = total(sums, "dp")
    sums, held[farthest] = lax.optimization_barrier((sums, held[farthest]))
    total_slots = peers(sums, "mp")
    for distance in reversed(nearer):
        for place, block in list(held.items()):
            if place ^ distance not in held:
                held[place ^ distance] = swap(block, "mp", distance)
    hidden_slots = [held[place] for place in range(shards)]
    normed = pl.pallas_call(
        functools.partial(norm_kernel, features),
        in_specs=[SCALAR] + [VECTOR] * (2 + shards),
        out_specs=VECTOR,
        out_shape=jax.ShapeDtypeStruct((features // LANES, rows, LANES), jnp.bfloat16),
        compiler_params=room(2),
        cost_estimate=cost(4 * rows * features, 4 * rows * features),
        name="norm",
    )(me, squares, gain, *hidden_slots)
    exact, delta, sums, means = project(
        me, ratio_ids, live_row, total_slots, normed, q_weight, kv_weight, float(tokens)
    )
    sums = sum(peers(sums, "mp"))
    *steps, final = distances("dp")
    for distance in steps:
        sums = sums + swap(sums, "dp", distance)
    losses, q_latent, kv_latent = pl.pallas_call(
        blend_kernel,
        in_specs=[VECTOR] * 4,
        out_shape=[
            jax.ShapeDtypeStruct((RATIOS,), jnp.float32),
            jax.ShapeDtypeStruct((rows, query), jnp.bfloat16),
            jax.ShapeDtypeStruct((rows, kv), jnp.bfloat16),
        ],
        out_specs=[SCALAR, VECTOR, VECTOR],
        compiler_params=room(2),
        cost_estimate=cost(10 * rows * (query + kv), 24 * rows * (query + kv)),
        name="blend",
    )(sums, swap(sums, "dp", final), exact, delta)
    return losses, q_latent, kv_latent, means.reshape(features)


def solution(mesh):
    placed = (P("dp", "mp"), P("dp"), P(), P(None, "mp"), P(None, "mp"), P())
    return jax.shard_map(
        per_device,
        mesh=mesh,
        in_specs=placed,
        out_specs=(P(), P("dp", "mp"), P("dp", "mp"), P()),
        check_vma=False,
    )
```

```python
import functools

import jax
import jax.numpy as jnp
from jax import lax
from jax.experimental import pallas as pl
from jax.experimental.pallas import tpu as pltpu
from jax.sharding import PartitionSpec as P

GROUP = 128
GRID = 20
RATIOS = 4
LANES = 128
HALF = 512
LINEAR, CONSTANT, GAIN = -1.1640625, 0.458984375, 8.705


def swap(x, axis, distance):
    size = lax.axis_size(axis)
    return lax.ppermute(x, axis, [(i, i ^ distance) for i in range(size)])


def distances(axis):
    size = lax.axis_size(axis)
    assert size & (size - 1) == 0
    return [1 << bit for bit in range(size.bit_length() - 1)]


def rounds(axis):
    masks = [[distance] for distance in distances(axis)]
    return [[1, 2, 3]] + masks[2:] if len(masks) > 1 else masks


def total(x, axis):
    for masks in rounds(axis):
        x = x + sum(swap(x, axis, mask) for mask in masks)
    return x


def peers(x, axis):
    return [x] + [swap(x, axis, distance) for distance in range(1, lax.axis_size(axis))]


def column(row):
    return jnp.transpose(jnp.broadcast_to(row, (LANES, LANES)))


def squares_kernel(hidden, squares, kept):
    kept[...] = hidden[...]
    for top in range(0, hidden.shape[0], LANES):
        gathered = jnp.zeros((LANES, LANES), jnp.float32)
        for at in range(0, hidden.shape[1], LANES):
            values = hidden[top : top + LANES, at : at + LANES].astype(jnp.float32)
            gathered = gathered + values * values
        squares[:, top : top + LANES] = jnp.sum(jnp.transpose(gathered), axis=0, keepdims=True)


def keep_kernel(squares, live, gain, mask, kept_gain):
    kept_gain[...] = gain[...]
    mask[...] = live[...].astype(jnp.float32)


def stats_kernel(features, me, squares, live, gain, hidden, sums):
    rows, width = hidden.shape
    per_slot = width // LANES
    for piece in range(per_slot):
        row = gain[pl.ds(me[0] * per_slot + piece, 1), :]
        gathered = jnp.zeros((1, LANES), jnp.float32)
        for top in range(0, rows, LANES):
            rooted = column(lax.rsqrt(squares[:, top : top + LANES] / features + 1e-06))
            mask = column(live[:, top : top + LANES])
            values = hidden[top : top + LANES, piece * LANES : (piece + 1) * LANES].astype(jnp.float32)
            values = (values * rooted * row).astype(jnp.bfloat16).astype(jnp.float32)
            gathered = gathered + jnp.sum(jnp.abs(values) * mask, axis=0, keepdims=True)
        sums[piece : piece + 1, :] = gathered


def norm_kernel(features, *refs):
    me, squares, gain, *hidden, normed = refs
    rows, width = hidden[0].shape
    per_slot = width // LANES
    for top in range(0, rows, LANES):
        mean_square = squares[:, top : top + LANES] / features
        rooted = column(lax.rsqrt(mean_square + 1e-06))
        for slot in range(len(hidden)):
            owner = me[0] ^ slot
            for piece in range(per_slot):
                place = owner * per_slot + piece
                values = hidden[slot][top : top + LANES, piece * LANES : (piece + 1) * LANES]
                values = values.astype(jnp.float32) * rooted * gain[pl.ds(place, 1), :]
                normed[place, top : top + LANES, :] = values.astype(jnp.bfloat16)


def project_kernel(count, tokens, *refs):
    me, ids, live = refs[:3]
    totals = refs[3 : 3 + count]
    normed, start_query, start_kv, query, kv = refs[3 + count : 8 + count]
    exact, delta, sums, means = refs[8 + count : 12 + count]
    scales, table, stretched, held, arrivals, waves = refs[12 + count :]
    rows = normed.shape[1]
    blocks = normed.shape[0]
    per_slot = blocks // count
    groups = HALF // GROUP
    parts = [(ref, at) for ref in (query, kv) for at in range(0, ref.shape[1], LANES)]
    steps = blocks // (2 * groups)

    def fetches(step):
        slot = lax.rem(step, 2)
        span = pl.ds(pl.multiple_of(step * 2 * HALF, 2 * HALF), 2 * HALF)
        return [
            pltpu.make_async_copy(ref.at[span, pl.ds(at, LANES)], held.at[slot, spot], arrivals.at[slot, spot])
            for spot, (ref, at) in enumerate(parts)
        ]

    def prepare(group, buffer):
        table[buffer] = jnp.transpose(scales[group])
        for ratio in range(RATIOS):
            stretched[buffer, ratio] = jnp.broadcast_to(table[buffer, :, ratio : ratio + 1], (LANES, LANES))

    def quantize(half, group, buffer, slot):
        top = half * HALF + group * GROUP
        for spot in range(len(parts)):
            wide = held[slot, spot, top : top + GROUP, :].astype(jnp.float32)
            for ratio in range(RATIOS):
                scaled = wide * stretched[buffer, ratio]
                peak = jnp.max(jnp.abs(scaled), axis=0, keepdims=True) + 1e-06
                level = scaled * (7.0 / peak)
                part = (level - jnp.round(level)).astype(jnp.bfloat16)
                square = part * part
                series = (square + jnp.bfloat16(LINEAR)) * square + jnp.bfloat16(CONSTANT)
                wave = series * (jnp.bfloat16(0.25) - square) * part
                wave = wave * (peak * (GAIN / 7.0)).astype(jnp.bfloat16)
                waves[half, ratio, spot, group * GROUP : (group + 1) * GROUP, :] = wave

    def multiply(half, first):
        for ratio in range(RATIOS):
            left = []
            for group in range(groups):
                shrink = scales[first + group, RATIOS + ratio : RATIOS + ratio + 1, :]
                left.append(normed[first + group] * shrink.astype(jnp.bfloat16))
            right = jnp.concatenate([waves[half, ratio, spot] for spot in range(len(parts))], axis=1)
            delta[ratio] += jnp.dot(jnp.concatenate(left, axis=1), right, preferred_element_type=jnp.float32)

    def project_exact(half, first, slot):
        left = jnp.concatenate([normed[first + group] for group in range(groups)], axis=1)
        right = [held[slot, spot, half * HALF : (half + 1) * HALF, :] for spot in range(len(parts))]
        exact[...] += jnp.dot(left, jnp.concatenate(right, axis=1), preferred_element_type=jnp.float32)

    starts = [(ref, at) for ref in (start_query, start_kv) for at in range(0, ref.shape[1], LANES)]
    for spot, (ref, at) in enumerate(starts):
        held[0, spot] = ref[:, at : at + LANES]
    for slot in range(count):
        owner = me[0] ^ slot
        for piece in range(per_slot):
            means[pl.ds(owner * per_slot + piece, 1), :] = totals[slot][piece : piece + 1, :]
    sums_all = means[...]
    logged = jnp.log(sums_all + 1e-06)
    centred = logged - 0.5 * (jnp.max(logged) + jnp.min(logged))
    means[...] = sums_all / tokens
    for ratio in range(RATIOS):
        alpha = ids[ratio].astype(jnp.float32) / GRID
        scale = jnp.exp(alpha * centred)
        scales[:, ratio, :] = scale
        scales[:, RATIOS + ratio, :] = 1.0 / scale
    exact[...] = jnp.zeros_like(exact)
    delta[...] = jnp.zeros_like(delta)
    waves[1] = jnp.zeros_like(waves[1])
    prepare(0, 0)

    @pl.loop(0, steps)
    def _(step):
        base = step * 2 * groups
        slot = lax.rem(step, 2)

        @pl.when(step + 1 < steps)
        def _():
            for fetch in fetches(step + 1):
                fetch.start()

        @pl.when(step > 0)
        def _():
            for fetch in fetches(step):
                fetch.wait()

        for half in range(2):
            first = base + half * groups
            for group in range(groups):
                index = half * groups + group
                prepare(jnp.minimum(base + index + 1, blocks - 1), (index + 1) % 2)
                quantize(half, group, index % 2, slot)
            multiply(1 - half, jnp.maximum(first - groups, 0))
            project_exact(half, first, slot)

    multiply(1, blocks - groups)
    masks = [column(live[:, top : top + LANES]) for top in range(0, rows, LANES)]
    for ratio in range(RATIOS + 1):
        gathered = jnp.zeros((1, LANES), jnp.float32)
        for index, top in enumerate(range(0, rows, LANES)):
            for at in range(0, exact.shape[1], LANES):
                if ratio < RATIOS:
                    value = delta[ratio, top : top + LANES, at : at + LANES]
                else:
                    value = exact[top : top + LANES, at : at + LANES]
                value = value * masks[index]
                gathered = gathered + jnp.sum(value * value, axis=0, keepdims=True)
        sums[ratio : ratio + 1, :] = gathered
    sums[RATIOS + 1 :, :] = jnp.zeros((8 - RATIOS - 1, LANES), jnp.float32)


def project_scoped(count, tokens, spots, *refs):
    def run(waves):
        project_kernel(count, tokens, *refs, waves)

    pl.run_scoped(run, pltpu.VMEM((2, RATIOS, spots, HALF, LANES), jnp.bfloat16))


def blend_kernel(first, second, exact, delta, losses, query, kv):
    sums = first[...] + second[...]
    folded = [jnp.sum(sums[ratio : ratio + 1, :], axis=1, keepdims=True) for ratio in range(RATIOS + 1)]
    loss = [folded[ratio] / folded[RATIOS] for ratio in range(RATIOS)]
    inverse = [1.0 / (value * value) for value in loss]
    whole = inverse[0]
    for ratio in range(1, RATIOS):
        whole = whole + inverse[ratio]
    blended = exact[...]
    for ratio in range(RATIOS):
        losses[ratio] = loss[ratio][0, 0]
        blended = blended - (inverse[ratio] / whole) * delta[ratio]
    blended = blended.astype(jnp.bfloat16)
    query[...] = blended[:, : query.shape[1]]
    kv[...] = blended[:, query.shape[1] :]


SCALAR = pl.BlockSpec(memory_space=pltpu.SMEM)
VECTOR = pl.BlockSpec(memory_space=pltpu.VMEM)


def room(mebibytes):
    return pltpu.CompilerParams(vmem_limit_bytes=mebibytes << 20)


def cost(flops, moved):
    return pl.CostEstimate(flops=flops, bytes_accessed=moved, transcendentals=0)


def project(me, ratio_ids, live, total_slots, normed, start, q_weight, kv_weight, tokens):
    blocks, rows, _ = normed.shape
    features = blocks * LANES
    columns = q_weight.shape[1] + kv_weight.shape[1]
    spots = columns // LANES
    count = len(total_slots)
    return pl.pallas_call(
        functools.partial(project_scoped, count, tokens, spots),
        in_specs=[SCALAR, SCALAR] + [VECTOR] * (4 + count) + [pl.BlockSpec(memory_space=pl.ANY)] * 2,
        out_specs=[VECTOR] * 4,
        out_shape=[
            jax.ShapeDtypeStruct((rows, columns), jnp.float32),
            jax.ShapeDtypeStruct((RATIOS, rows, columns), jnp.float32),
            jax.ShapeDtypeStruct((8, LANES), jnp.float32),
            jax.ShapeDtypeStruct((blocks, LANES), jnp.float32),
        ],
        scratch_shapes=[
            pltpu.VMEM((blocks, 8, LANES), jnp.float32),
            pltpu.VMEM((2, LANES, 8), jnp.float32),
            pltpu.VMEM((2, RATIOS, LANES, LANES), jnp.float32),
            pltpu.VMEM((2, spots, 2 * HALF, LANES), jnp.bfloat16),
            pltpu.SemaphoreType.DMA((2, spots)),
        ],
        compiler_params=room(49),
        cost_estimate=cost(10 * rows * features * columns, 8 * features * columns),
        name="project",
    )(me, ratio_ids, live, *total_slots, normed, *start, q_weight, kv_weight)


def per_device(hidden, live, norm_gain, q_weight, kv_weight, ratio_ids):
    rows, width = hidden.shape
    shards = lax.axis_size("mp")
    features = width * shards
    tokens = rows * lax.axis_size("dp")
    query, kv = q_weight.shape[1], kv_weight.shape[1]
    me = lax.axis_index("mp").reshape(1).astype(jnp.int32)

    squares, hidden = pl.pallas_call(
        squares_kernel,
        in_specs=[VECTOR],
        out_specs=[VECTOR] * 2,
        out_shape=[
            jax.ShapeDtypeStruct((1, rows), jnp.float32),
            jax.ShapeDtypeStruct(hidden.shape, hidden.dtype),
        ],
        compiler_params=room(2),
        cost_estimate=cost(2 * rows * width, 4 * rows * width),
        name="squares",
    )(hidden)
    live_row, gain = pl.pallas_call(
        keep_kernel,
        in_specs=[VECTOR] * 3,
        out_specs=[VECTOR] * 2,
        out_shape=[
            jax.ShapeDtypeStruct((1, rows), jnp.float32),
            jax.ShapeDtypeStruct((features // LANES, LANES), jnp.float32),
        ],
        compiler_params=room(2),
        cost_estimate=cost(2 * rows * width, 4 * rows * width),
        name="keep",
    )(squares, live.reshape(1, rows), norm_gain.reshape(features // LANES, LANES))
    parts, live_row, gain = lax.optimization_barrier((peers(squares, "mp"), live_row, gain))
    squares = sum(parts)
    squares, late = lax.optimization_barrier((squares, hidden))
    *nearer, farthest = distances("mp")
    held = {0: late, farthest: swap(late, "mp", farthest)}
    for distance in nearer:
        held[distance] = swap(late, "mp", distance)
    sums = pl.pallas_call(
        functools.partial(stats_kernel, features),
        in_specs=[SCALAR] + [VECTOR] * 4,
        out_specs=VECTOR,
        out_shape=jax.ShapeDtypeStruct((width // LANES, LANES), jnp.float32),
        compiler_params=room(2),
        cost_estimate=cost(8 * rows * width, 2 * rows * width),
        name="stats",
    )(me, squares, live_row, gain, hidden)
    first, *others = rounds("dp")
    sums = sums + sum(swap(sums, "dp", mask) for mask in first)
    for distance in nearer:
        sums, held[distance] = lax.optimization_barrier((sums, held[distance]))
    for masks in others:
        sums = sums + sum(swap(sums, "dp", mask) for mask in masks)
    block = 2 * HALF
    sums, held[farthest], *start = lax.optimization_barrier(
        (sums, held[farthest], q_weight[:block], kv_weight[:block])
    )
    total_slots = peers(sums, "mp")
    for distance in reversed(nearer):
        for place, block in list(held.items()):
            if place ^ distance not in held:
                held[place ^ distance] = swap(block, "mp", distance)
    hidden_slots = [held[place] for place in range(shards)]
    normed = pl.pallas_call(
        functools.partial(norm_kernel, features),
        in_specs=[SCALAR] + [VECTOR] * (2 + shards),
        out_specs=VECTOR,
        out_shape=jax.ShapeDtypeStruct((features // LANES, rows, LANES), jnp.bfloat16),
        compiler_params=room(2),
        cost_estimate=cost(4 * rows * features, 4 * rows * features),
        name="norm",
    )(me, squares, gain, *hidden_slots)
    exact, delta, sums, means = project(
        me, ratio_ids, live_row, total_slots, normed, start, q_weight, kv_weight, float(tokens)
    )
    sums = sum(peers(sums, "mp"))
    *steps, final = rounds("dp")
    for masks in steps:
        sums = sums + sum(swap(sums, "dp", mask) for mask in masks)
    losses, q_latent, kv_latent = pl.pallas_call(
        blend_kernel,
        in_specs=[VECTOR] * 4,
        out_shape=[
            jax.ShapeDtypeStruct((RATIOS,), jnp.float32),
            jax.ShapeDtypeStruct((rows, query), jnp.bfloat16),
            jax.ShapeDtypeStruct((rows, kv), jnp.bfloat16),
        ],
        out_specs=[SCALAR, VECTOR, VECTOR],
        compiler_params=room(2),
        cost_estimate=cost(10 * rows * (query + kv), 24 * rows * (query + kv)),
        name="blend",
    )(sums, sum(swap(sums, "dp", mask) for mask in final), exact, delta)
    return losses, q_latent, kv_latent, means.reshape(features)


def solution(mesh):
    placed = (P("dp", "mp"), P("dp"), P(), P(None, "mp"), P(None, "mp"), P())
    return jax.shard_map(
        per_device,
        mesh=mesh,
        in_specs=placed,
        out_specs=(P(), P("dp", "mp"), P("dp", "mp"), P()),
        check_vma=False,
    )
```
